32 devices in a mesh: dp: 8 (over y, x, core), mp: 4 (over z).
Axes of the slice: x: 2, y: 2, z: 4, core: 2. Of those that a mesh axis runs over, the one named last changes fastest.
Arguments:
- states: bfloat16 [128, 80, 768], P('dp'), may hold values from -6 to 6
- hist_len: int32 [128], P('dp'), may hold values from 1 to 20
- norm_gain: float32 [768], replicated, may hold values from 0.5 to 1.5
- qkv_weight: bfloat16 [768, 3, 12, 64], P(None, None, 'mp'), may hold values from -1 to 1
- output_weight: bfloat16 [12, 64, 768], P('mp'), may hold values from -0.21875 to 0.21875
- cotangent: bfloat16 [128, 80, 768], P('dp'), may hold values from -6 to 6
Outputs:
- attended: bfloat16 [128, 80, 768], P('dp')
- grad_states: bfloat16 [128, 80, 768], P('dp')
- grad_qkv: float32 [768, 3, 12, 64], P('dp', None, 'mp')
- output_weight_gradient: float32 [12, 64, 768], P('mp', None, 'dp')
- grad_gain: float32 [768], P('dp')
The draws below stay inside these ranges and needn't reach their ends.
All inputs are finite; a program needn't handle non-finite values.
Results may differ from the reference program's by a relative error of at most 0.012.
Values may be sent and summed in bfloat16 or wider, within the bound.
No kernel may reach another device: no remote copies, remote signals or barrier semaphores. Data moves between devices by JAX's collectives and lax.ppermute only.
A program may use at most 128 MiB of HBM per device.

```python
import jax
import jax.numpy as jnp
from jax import lax

D = 768
H = 12
DH = 64
ITEMS = 20
LEVELS = 4
S = 80
B = 128


def draw_qkv_weight(key, part):
    k_base, k_noise, k_value = jax.random.split(key, 3)
    inverse = D ** (-0.5)
    query_part = 0.5 * inverse * jax.random.normal(k_base, (D, H, DH), jnp.float32)
    key_part = 0.5 * inverse * jax.random.normal(k_noise, (D, H, DH), jnp.float32)
    value_part = inverse * jax.random.normal(k_value, (D, H, DH), jnp.float32)
    stacked = jnp.stack([query_part, key_part, value_part], axis=1)
    return jnp.clip(stacked, -1.0, 1.0).astype(jnp.bfloat16)


def set_ends(drawn, own_key, least, high):
    longest = drawn.shape.index(max(drawn.shape))
    spots = []
    for shift in (0, 1):
        where = [jax.random.randint(jax.random.fold_in(own_key, axis), (), 0, length) for axis, length in enumerate(drawn.shape)]
        where[longest] = (where[longest] + shift) % drawn.shape[longest]
        spots.append(tuple(where))
    return drawn.at[spots[0]].set(least).at[spots[1]].set(high)


def with_spikes(drawn, key, source, target, blocks, factor):
    def block_of(dim):
        return (jnp.arange(drawn.shape[dim]) // (drawn.shape[dim] // blocks)).reshape((-1,) + (1,) * (drawn.ndim - 1 - dim))

    first = jax.random.permutation(key, blocks)[block_of(target)]
    far = (block_of(target) + blocks // 2) % blocks
    return jnp.where((block_of(source) == first) | (block_of(source) == far), factor * drawn, drawn)


def block_levels(stream_key, extent, cuts, smallest, high):
    level, own = 1.0, jax.random.fold_in(stream_key, 6)
    for dim, blocks in cuts:
        heights = jnp.exp(jax.random.uniform(jax.random.fold_in(own, dim), (blocks,), jnp.float32, smallest / len(cuts), high / len(cuts)))
        level = level * jnp.repeat(heights, extent[dim] // blocks).reshape([-1 if axis == dim else 1 for axis in range(len(extent))])
    return level


def gaussian(own_key, shape, deviation, limit, pieces=(), kind=jnp.bfloat16):
    array = jax.random.normal(own_key, shape, jnp.float32) * deviation
    if len(pieces) > 0:
        array = block_levels(own_key, shape, pieces, -0.22, 0.18) * array
    return jnp.clip(array, min=-limit, max=limit).astype(kind)


def gaussian_with(rng, shape, deviation, reach, cuts, heavy, kind=jnp.bfloat16):
    result = deviation * jax.random.normal(rng, shape, jnp.float32)
    if cuts:
        result = result * block_levels(rng, shape, cuts, -0.22, 0.18)
    return jnp.clip(with_spikes(result, jax.random.fold_in(rng, 3), *heavy), -reach, reach).astype(kind)


def setup_inputs(seed: int = 0) -> dict:
    keys = jax.random.split(jax.random.key(seed), 7)
    states = gaussian_with(keys[0], (B, S, D), 1.0, 6.0, ((0, 8),), (0, 2, 8, 2.0))
    hist_len = set_ends(jax.random.randint(keys[1], (B,), 1, ITEMS + 1), jax.random.fold_in(keys[1], 1), 1, ITEMS).astype(jnp.int32)
    norm_gain = jnp.clip(1.0 + 0.1 * jax.random.normal(keys[2], (D,), jnp.float32), 0.5, 1.5)
    qkv_weight = draw_qkv_weight(jax.random.fold_in(keys[6], 71), 0)
    output_weight = gaussian(keys[4], (H, DH, D), (H * DH) ** -0.5, 0.21875, ((0, 4),))
    cotangent = gaussian_with(keys[5], (B, S, D), 1.0, 6.0, ((0, 8),), (0, 2, 8, 2.0))
    return {"states": states, "hist_len": hist_len, "norm_gain": norm_gain, "qkv_weight": qkv_weight, "output_weight": output_weight, "cotangent": cotangent}


def reference(states, hist_len, norm_gain, qkv_weight, output_weight, cotangent):
    wide_states = states.astype(jnp.float32)
    inv_rms = lax.rsqrt(lax.optimization_barrier(jnp.mean(wide_states * wide_states, axis=-1, keepdims=True)) + 1e-06)
    unit = wide_states * inv_rms
    normed = (unit * norm_gain).astype(jnp.bfloat16)
    proj = jnp.einsum('bsd,dchk->bschk', normed.astype(jnp.float32), qkv_weight.astype(jnp.float32)).astype(jnp.bfloat16)
    queries = proj[:, :, 0].astype(jnp.float32)
    key_rows = proj[:, :, 1].astype(jnp.float32)
    value_rows = proj[:, :, 2].astype(jnp.float32)
    positions = jnp.arange(states.shape[1], dtype=jnp.int32)
    keep_mask = positions[None, :] < LEVELS * hist_len[:, None]
    scores = jnp.einsum('bqhk,bphk->bhqp', queries, key_rows)
    masked = jnp.where(keep_mask[:, None, None, :], scores, -1e+30)
    row_top = lax.optimization_barrier(jnp.max(masked, axis=-1, keepdims=True))
    exp_scores = jnp.exp(masked - row_top)
    attn_prob = exp_scores / lax.optimization_barrier(jnp.sum(exp_scores, axis=-1, keepdims=True))
    prob_bf = attn_prob.astype(jnp.bfloat16).astype(jnp.float32)
    attended_context = jnp.einsum('bhqp,bphk->bqhk', prob_bf, value_rows).astype(jnp.bfloat16)
    mixed_total_sum = jnp.einsum('zagm,gms->zas', attended_context.astype(jnp.float32), output_weight.astype(jnp.float32))
    attended = (wide_states + mixed_total_sum).astype(jnp.bfloat16)
    masked_cotangent = jnp.where(keep_mask[:, :, None], cotangent, jnp.zeros_like(cotangent)).astype(jnp.float32)
    output_weight_gradient = jnp.einsum('wmep,wmx->epx', attended_context.astype(jnp.float32), masked_cotangent)
    context_gradient = jnp.einsum('uxy,wgy->uxwg', masked_cotangent, output_weight.astype(jnp.float32)).astype(jnp.bfloat16).astype(jnp.float32)
    grad_prob = jnp.einsum('bqhk,bphk->bhqp', context_gradient, value_rows)
    row_delta = lax.optimization_barrier(jnp.sum(attn_prob * grad_prob, axis=-1, keepdims=True))
    grad_score = (attn_prob * (grad_prob - row_delta)).astype(jnp.bfloat16).astype(jnp.float32)
    grad_query = jnp.einsum('bhqp,bphk->bqhk', grad_score, key_rows)
    grad_key = jnp.einsum('bhqp,bqhk->bphk', grad_score, queries)
    grad_value = jnp.einsum('bhqp,bqhk->bphk', prob_bf, context_gradient)
    grad_proj = jnp.stack([grad_query, grad_key, grad_value], axis=2).astype(jnp.bfloat16).astype(jnp.float32)
    grad_qkv = jnp.einsum('bsd,bschk->dchk', normed.astype(jnp.float32), grad_proj)
    grad_normed = jnp.einsum('bschk,dchk->bsd', grad_proj, qkv_weight.astype(jnp.float32))
    grad_gain = lax.optimization_barrier(jnp.sum(grad_normed * unit, axis=(0, 1)))
    grad_unit = grad_normed * norm_gain
    row_corr = lax.optimization_barrier(jnp.mean(grad_unit * unit, axis=-1, keepdims=True))
    grad_states = (masked_cotangent + inv_rms * (grad_unit - unit * row_corr)).astype(jnp.bfloat16)
    return (attended, grad_states, grad_qkv, output_weight_gradient, grad_gain)
```

```python
import functools

import jax
import jax.numpy as jnp
from jax import lax
from jax.experimental import pallas as pl
from jax.experimental.pallas import tpu as pltpu
from jax.sharding import PartitionSpec as P

LEVELS = 4
EPS = 1e-06
F32 = jnp.float32
BF16 = jnp.bfloat16


def dot_nt(a, b):
    return lax.dot_general(a, b, (((1,), (1,)), ((), ())), preferred_element_type=F32)


def dot_nn(a, b):
    return lax.dot_general(a, b, (((1,), (0,)), ((), ())), preferred_element_type=F32)


def dot_tn(a, b):
    return lax.dot_general(a, b, (((0,), (0,)), ((), ())), preferred_element_type=F32)


def attention(q, k, v, g, valid, heads, width):
    seq = q.shape[0]
    lane_head = lax.broadcasted_iota(jnp.int32, (1, heads * width), 1) // width
    masks = [(lane_head == h).astype(BF16) for h in range(heads)]
    q_blocks = jnp.concatenate([q * m for m in masks], axis=0)
    g_blocks = jnp.concatenate([g * m for m in masks], axis=0)
    scores = dot_nt(k, q_blocks)
    row = lax.broadcasted_iota(jnp.int32, scores.shape, 0)
    scores = jnp.where(row < valid, scores, -1e30)
    top = jnp.max(scores, axis=0, keepdims=True)
    exp_scores = jnp.exp(scores - top)
    prob = exp_scores * (1.0 / jnp.sum(exp_scores, axis=0, keepdims=True))
    prob_bf = prob.astype(BF16)
    grad_prob = dot_nt(v, g_blocks)
    delta = jnp.sum(prob * grad_prob, axis=0, keepdims=True)
    grad_scores = (prob * (grad_prob - delta)).astype(BF16)
    grad_v = dot_nn(prob_bf, g_blocks)
    grad_k = dot_nn(grad_scores, q_blocks)

    def diagonal(full):
        out = full[:seq]
        for h in range(1, heads):
            out = jnp.where(lane_head == h, full[h * seq : (h + 1) * seq], out)
        return out

    context = diagonal(dot_tn(prob_bf, v))
    grad_q = diagonal(dot_tn(grad_scores, k))
    return grad_q, grad_k, grad_v, context


def keep_rows(len_ref, first, count, seq):
    rows = [lax.broadcasted_iota(jnp.int32, (seq, 1), 0) < LEVELS * len_ref[first + b] for b in range(count)]
    return jnp.concatenate([r.astype(F32) for r in rows], axis=0)


def shard_body(len_ref, normed, mcot, w_q, w_k, w_v, w_o, out_ref, scratch, seq, heads, width):
    q_s, k_s, v_s, g_s = scratch
    chunk = pl.program_id(0)
    count = normed.shape[0] // seq
    q_s[...] = dot_nt(normed, w_q).astype(BF16)
    k_s[...] = dot_nt(normed, w_k).astype(BF16)
    v_s[...] = dot_nt(normed, w_v).astype(BF16)
    g_s[...] = dot_nt(mcot, w_o).astype(BF16)
    for b in range(count):
        rows = slice(b * seq, (b + 1) * seq)
        valid = LEVELS * len_ref[chunk * count + b]
        parts = attention(q_s[rows], k_s[rows], v_s[rows], g_s[rows], valid, heads, width)
        for n, part in enumerate(parts):
            out_ref[0, n, rows] = part.astype(BF16)


def own_kernel(seq, heads, width, len_ref, meta_ref, states_ref, cot_ref, gain_ref, qkv_ref, wo_ref,
               normed_ref, mcot_ref, out_ref, wt_ref, q_s, k_s, v_s, g_s):
    wide = states_ref[...].astype(F32)
    inv = lax.rsqrt(jnp.mean(wide * wide, axis=-1, keepdims=True) + EPS)
    normed = (wide * inv * gain_ref[...]).astype(BF16)
    normed_ref[...] = normed
    count = normed.shape[0] // seq
    keep = keep_rows(len_ref, pl.program_id(0) * count, count, seq)
    mcot = (cot_ref[...].astype(F32) * keep).astype(BF16)
    mcot_ref[...] = mcot
    n = heads * width

    @pl.when(pl.program_id(0) == 0)
    def _():
        wt_ref[0, : 3 * n] = qkv_ref[...]
        wt_ref[0, 3 * n :] = wo_ref[...]

    shard_body(len_ref, normed, mcot, qkv_ref[:n], qkv_ref[n : 2 * n], qkv_ref[2 * n : 3 * n], wo_ref[...],
               out_ref, (q_s, k_s, v_s, g_s), seq, heads, width)


def far_kernel(seq, heads, width, parts, len_ref, meta_ref, normed_ref, mcot_ref, *refs):
    blocks, (old_out, old_wt) = refs[:parts], refs[parts : parts + 2]
    out_ref, wt_ref, q_s, k_s, v_s, g_s, sems = refs[parts + 2 :]
    n = heads * width
    size = 4 * n // parts

    @pl.when(pl.program_id(0) == 0)
    def _():
        copies = []
        for r in range(parts):
            place = pl.multiple_of((meta_ref[1] ^ r) * size, 8)
            copies.append(pltpu.make_async_copy(blocks[r], wt_ref.at[0, pl.ds(place, size)], sems.at[r]))
        for copy in copies:
            copy.start()
        for copy in copies:
            copy.wait()

    w = [wt_ref[0, i * n : (i + 1) * n] for i in range(4)]
    shard_body(len_ref, normed_ref[...], mcot_ref[...], w[0], w[1], w[2], w[3],
               out_ref, (q_s, k_s, v_s, g_s), seq, heads, width)


def weight_grad_kernel(parts, n, len_ref, meta_ref, normed_ref, mcot_ref, all_ref, *refs):
    outs, acc = refs[:parts], refs[parts]
    step = pl.program_id(0)
    rows = normed_ref.shape[1]
    size = outs[0].shape[0]
    per = rows // size
    for i in range(4):
        left = mcot_ref[...] if i == 3 else normed_ref[...]
        piece = dot_tn(left, all_ref[0, i])
        for c in range(per):
            acc[i, step * per + c] = piece[c * size : (c + 1) * size]

    @pl.when(step == pl.num_programs(0) - 1)
    def _():
        for r in range(parts):
            for i in range(4):
                outs[r][:, i * n : (i + 1) * n] = acc[i, meta_ref[1] ^ r].astype(outs[r].dtype)


def out_kernel(seq, n, shards, len_ref, meta_ref, states_ref, mcot_ref, gain_ref, all_ref, wt_ref,
               att_ref, grad_ref, gain_out_ref):
    total = None
    grad = None
    for s in range(shards):
        piece = dot_nn(all_ref[s, 3], wt_ref[s, 3 * n :])
        total = piece if total is None else total + piece
        for i in range(3):
            piece = dot_nn(all_ref[s, i], wt_ref[s, i * n : (i + 1) * n])
            grad = piece if grad is None else grad + piece
    wide = states_ref[...].astype(F32)
    inv = lax.rsqrt(jnp.mean(wide * wide, axis=-1, keepdims=True) + EPS)
    unit = wide * inv
    att_ref[...] = (wide + total).astype(BF16)

    @pl.when(pl.program_id(0) == 0)
    def _():
        gain_out_ref[...] = jnp.zeros_like(gain_out_ref)

    gain_out_ref[...] += jnp.sum(grad * unit, axis=0, keepdims=True)
    unit_grad = grad * gain_ref[...]
    corr = jnp.mean(unit_grad * unit, axis=-1, keepdims=True)
    grad_ref[...] = (mcot_ref[...].astype(F32) + inv * (unit_grad - unit * corr)).astype(BF16)


def body(dp, mp, states, hist_len, norm_gain, qkv_weight, output_weight, cotangent):
    batch, seq, d = states.shape
    _, _, heads, width = qkv_weight.shape
    n = heads * width
    rows = batch * seq
    parts = 8
    low = dp // parts
    i_dp = lax.axis_index("dp")
    i_hi = i_dp // low
    i_mp = lax.axis_index("mp")

    def hop_dp(x, r):
        return lax.ppermute(x, "dp", [(i, i ^ (r * low)) for i in range(dp)])

    def hop_mp(x, k):
        return lax.ppermute(x, "mp", [(i, i ^ k) for i in range(mp)])

    qkv_rows = jnp.transpose(qkv_weight, (1, 2, 3, 0)).reshape(3 * n, d)
    wo_rows = output_weight.reshape(n, d)
    stacked = jnp.concatenate([qkv_rows, wo_rows], axis=0)
    size = 4 * n // parts
    mine = lax.dynamic_slice_in_dim(stacked, i_hi * size, size, 0)

    gathered = []
    for k in range(1, mp):
        first = hop_mp(mine, k)
        even = {0: first}
        for r in range(2, parts, 2):
            even[r] = hop_dp(first, r)
        blocks = dict(even)
        for r in range(0, parts, 2):
            blocks[r ^ 1] = hop_dp(even[r], 1)
        gathered.append([blocks[r] for r in range(parts)])

    flat_states = states.reshape(rows, d)
    flat_cot = cotangent.reshape(rows, d)
    gain = norm_gain.reshape(1, d)
    chunk = rows // 4
    grid = rows // chunk
    vmem = 60 * 1024 * 1024
    scratch = [pltpu.VMEM((chunk, n), BF16) for _ in range(4)]
    flops_in = 2 * rows * d * 4 * n
    cost = pl.CostEstimate(flops=3 * flops_in, bytes_accessed=rows * d * 8, transcendentals=0)
    row_spec = pl.BlockSpec((chunk, d), lambda c, *_: (c, 0))
    all_spec = pl.BlockSpec((1, 4, chunk, n), lambda c, length, meta: (meta[0], 0, c, 0))
    wt_spec = pl.BlockSpec((1, 4 * n, d), lambda c, length, meta: (meta[0], 0, 0))
    any_spec = pl.BlockSpec(memory_space=pl.ANY)
    all_shape = jax.ShapeDtypeStruct((mp, 4, rows, n), BF16)
    wt_shape = jax.ShapeDtypeStruct((mp, 4 * n, d), BF16)
    params = pltpu.CompilerParams(dimension_semantics=("arbitrary",), vmem_limit_bytes=vmem)

    def meta_of(shard):
        return jnp.stack([shard, i_hi]).astype(jnp.int32)

    whole = lambda shape: pl.BlockSpec(shape, lambda c, *_: tuple(0 for _ in shape))
    normed, mcot, everything, weights = pl.pallas_call(
        functools.partial(own_kernel, seq, heads, width),
        grid_spec=pltpu.PrefetchScalarGridSpec(
            num_scalar_prefetch=2, grid=(grid,),
            in_specs=[row_spec, row_spec, whole((1, d)), whole((3 * n, d)), whole((n, d))],
            out_specs=[row_spec, row_spec, all_spec, wt_spec],
            scratch_shapes=scratch),
        out_shape=[jax.ShapeDtypeStruct((rows, d), BF16)] * 2 + [all_shape, wt_shape],
        compiler_params=params, cost_estimate=cost, name="own_shard",
    )(hist_len, meta_of(i_mp), flat_states, flat_cot, gain, qkv_rows, wo_rows)

    pieces = pl.pallas_call(
        functools.partial(weight_grad_kernel, parts, n),
        grid_spec=pltpu.PrefetchScalarGridSpec(
            num_scalar_prefetch=2, grid=(2,),
            in_specs=[pl.BlockSpec((rows, d // 2), lambda c, *_: (0, c)),
                      pl.BlockSpec((rows, d // 2), lambda c, *_: (0, c)),
                      pl.BlockSpec((1, 4, rows, n), lambda c, length, meta: (meta[0], 0, 0, 0))],
            out_specs=[whole((d // parts, 4 * n))] * parts,
            scratch_shapes=[pltpu.VMEM((4, parts, d // parts, n), F32)]),
        out_shape=[jax.ShapeDtypeStruct((d // parts, 4 * n), F32 if r == 0 else BF16) for r in range(parts)],
        compiler_params=params, cost_estimate=pl.CostEstimate(flops=flops_in, bytes_accessed=rows * d * 8, transcendentals=0),
        name="weight_grad",
    )(hist_len, meta_of(i_mp), normed, mcot, everything)
    arrived = [hop_dp(pieces[r], r) for r in range(1, parts)]

    for k in range(1, mp):
        everything, weights = pl.pallas_call(
            functools.partial(far_kernel, seq, heads, width, parts),
            grid_spec=pltpu.PrefetchScalarGridSpec(
                num_scalar_prefetch=2, grid=(grid,),
                in_specs=[row_spec, row_spec] + [any_spec] * (parts + 2),
                out_specs=[all_spec, wt_spec],
                scratch_shapes=scratch + [pltpu.SemaphoreType.DMA((parts,))]),
            out_shape=[all_shape, wt_shape],
            input_output_aliases={4 + parts: 0, 5 + parts: 1},
            compiler_params=params, cost_estimate=cost, name=f"far_shard_{k}",
        )(hist_len, meta_of(i_mp ^ k), normed, mcot, *gathered[k - 1], everything, weights)

    attended, grad_states, gain_part = pl.pallas_call(
        functools.partial(out_kernel, seq, n, mp),
        grid_spec=pltpu.PrefetchScalarGridSpec(
            num_scalar_prefetch=2, grid=(grid,),
            in_specs=[row_spec, row_spec, whole((1, d)),
                      pl.BlockSpec((mp, 4, chunk, n), lambda c, *_: (0, 0, c, 0)),
                      pl.BlockSpec((mp, 4 * n, d), lambda c, *_: (0, 0, 0), pipeline_mode=pl.Buffered(1))],
            out_specs=[row_spec, row_spec, whole((1, d))]),
        out_shape=[jax.ShapeDtypeStruct((rows, d), BF16)] * 2 + [jax.ShapeDtypeStruct((1, d), F32)],
        compiler_params=params,
        cost_estimate=pl.CostEstimate(flops=4 * flops_in, bytes_accessed=rows * d * 24, transcendentals=0),
        name="outputs",
    )(hist_len, meta_of(i_mp), flat_states, mcot, gain, everything, weights)

    summed = pieces[0]
    for piece in arrived:
        summed = summed + piece.astype(F32)
    gain_sum = gain_part
    for r in range(1, parts):
        gain_sum = gain_sum + hop_dp(gain_part, r)
    gain_piece = lax.dynamic_slice_in_dim(gain_sum.reshape(d), i_hi * (d // parts), d // parts, 0)
    if low > 1:
        groups = [[hi * low + lo for lo in range(low)] for hi in range(parts)]
        summed = lax.psum_scatter(summed, "dp", scatter_dimension=0, axis_index_groups=groups, tiled=True)
        gain_piece = lax.psum_scatter(gain_piece, "dp", scatter_dimension=0, axis_index_groups=groups, tiled=True)
    across = summed.T
    grad_qkv = jnp.transpose(across[: 3 * n].reshape(3, heads, width, -1), (3, 0, 1, 2))
    grad_output = across[3 * n :].reshape(heads, width, -1)
    return (attended.reshape(batch, seq, d), grad_states.reshape(batch, seq, d), grad_qkv, grad_output, gain_piece)


def solution(mesh):
    placed = (
        P("dp", None, None),
        P("dp"),
        P(),
        P(None, None, "mp", None),
        P("mp", None, None),
        P("dp", None, None),
    )
    return jax.shard_map(
        functools.partial(body, mesh.shape["dp"], mesh.shape["mp"]),
        mesh=mesh,
        in_specs=placed,
        out_specs=(
            P("dp", None, None),
            P("dp", None, None),
            P("dp", None, "mp", None),
            P("mp", None, "dp"),
            P("dp"),
        ),
        check_vma=False,
    )
```

```python
import functools

import jax
import jax.numpy as jnp
from jax import lax
from jax.experimental import pallas as pl
from jax.experimental.pallas import tpu as pltpu
from jax.sharding import PartitionSpec as P


LEVELS = 4
EPS = 1e-06
F32 = jnp.float32
BF16 = jnp.bfloat16


def dot_nt(a, b):
    return lax.dot_general(a, b, (((1,), (1,)), ((), ())), preferred_element_type=F32)


def dot_nn(a, b):
    return lax.dot_general(a, b, (((1,), (0,)), ((), ())), preferred_element_type=F32)


def dot_tn(a, b):
    return lax.dot_general(a, b, (((0,), (0,)), ((), ())), preferred_element_type=F32)


def attention(q, k, v, g, valid, heads, width):
    seq = q.shape[0]
    lane_head = lax.broadcasted_iota(jnp.int32, (1, heads * width), 1) // width
    masks = [(lane_head == h).astype(BF16) for h in range(heads)]
    q_blocks = jnp.concatenate([q * m for m in masks], axis=0)
    g_blocks = jnp.concatenate([g * m for m in masks], axis=0)
    scores = dot_nt(k, q_blocks)
    row = lax.broadcasted_iota(jnp.int32, scores.shape, 0)
    scores = jnp.where(row < valid, scores, -1e30)
    top = jnp.max(scores, axis=0, keepdims=True)
    exp_scores = jnp.exp(scores - top)
    prob = exp_scores * (1.0 / jnp.sum(exp_scores, axis=0, keepdims=True))
    prob_bf = prob.astype(BF16)
    grad_prob = dot_nt(v, g_blocks)
    delta = jnp.sum(prob * grad_prob, axis=0, keepdims=True)
    grad_scores = (prob * (grad_prob - delta)).astype(BF16)
    grad_v = dot_nn(prob_bf, g_blocks)
    grad_k = dot_nn(grad_scores, q_blocks)

    def diagonal(full):
        out = full[:seq]
        for h in range(1, heads):
            out = jnp.where(lane_head == h, full[h * seq : (h + 1) * seq], out)
        return out

    context = diagonal(dot_tn(prob_bf, v))
    grad_q = diagonal(dot_tn(grad_scores, k))
    return grad_q, grad_k, grad_v, context


def keep_rows(len_ref, first, count, seq):
    rows = [lax.broadcasted_iota(jnp.int32, (seq, 1), 0) < LEVELS * len_ref[first + b] for b in range(count)]
    return jnp.concatenate([r.astype(F32) for r in rows], axis=0)


def shard_body(len_ref, normed, mcot, w_q, w_k, w_v, w_o, out_ref, scratch, seq, heads, width):
    q_s, k_s, v_s, g_s = scratch
    chunk = pl.program_id(0)
    count = normed.shape[0] // seq
    q_s[...] = dot_nt(normed, w_q).astype(BF16)
    k_s[...] = dot_nt(normed, w_k).astype(BF16)
    v_s[...] = dot_nt(normed, w_v).astype(BF16)
    g_s[...] = dot_nt(mcot, w_o).astype(BF16)
    for b in range(count):
        rows = slice(b * seq, (b + 1) * seq)
        valid = LEVELS * len_ref[chunk * count + b]
        parts = attention(q_s[rows], k_s[rows], v_s[rows], g_s[rows], valid, heads, width)
        for n, part in enumerate(parts):
            out_ref[n, rows] = part.astype(BF16)


def own_kernel(seq, heads, width, len_ref, states_ref, cot_ref, gain_ref, qkv_ref, wo_ref,
               normed_ref, mcot_ref, out_ref, *scratch):
    wide = states_ref[...].astype(F32)
    inv = lax.rsqrt(jnp.mean(wide * wide, axis=-1, keepdims=True) + EPS)
    normed = (wide * inv * gain_ref[...]).astype(BF16)
    normed_ref[...] = normed
    count = normed.shape[0] // seq
    keep = keep_rows(len_ref, pl.program_id(0) * count, count, seq)
    mcot = (cot_ref[...].astype(F32) * keep).astype(BF16)
    mcot_ref[...] = mcot
    n = heads * width
    shard_body(len_ref, normed, mcot, qkv_ref[:n], qkv_ref[n : 2 * n], qkv_ref[2 * n : 3 * n], wo_ref[...],
               out_ref.at[:], scratch, seq, heads, width)


def far_kernel(seq, heads, width, parts, len_ref, meta_ref, normed_ref, mcot_ref, *refs):
    blocks = refs[:parts]
    out_ref, wt_ref, q_s, k_s, v_s, g_s, sems = refs[parts:]
    n = heads * width
    size = 4 * n // parts

    @pl.when(pl.program_id(0) == 0)
    def _():
        copies = []
        for r in range(parts):
            place = pl.multiple_of((meta_ref[1] ^ r) * size, 8)
            copies.append(pltpu.make_async_copy(blocks[r], wt_ref.at[pl.ds(place, size)], sems.at[r]))
        for copy in copies:
            copy.start()
        for copy in copies:
            copy.wait()

    w = [wt_ref[i * n : (i + 1) * n] for i in range(4)]
    shard_body(len_ref, normed_ref[...], mcot_ref[...], w[0], w[1], w[2], w[3],
               out_ref.at[:], (q_s, k_s, v_s, g_s), seq, heads, width)


def weight_grad_kernel(parts, n, meta_ref, normed_ref, mcot_ref, all_ref, *refs):
    outs, acc = refs[:-1], refs[-1]
    step = pl.program_id(0)
    rows = normed_ref.shape[1]
    size = rows * pl.num_programs(0) // parts
    per = parts // 2
    for i in range(4):
        left = mcot_ref[...] if i == 3 else normed_ref[...]
        piece = dot_tn(left, all_ref[i])
        for c in range(per):
            acc[i, step * per + c] = piece[c * size : (c + 1) * size]

    @pl.when(step == pl.num_programs(0) - 1)
    def _():
        for r in range(parts):
            for i in range(4):
                value = acc[i, meta_ref[1] ^ r]
                if r % 2 == 0:
                    outs[r // 2][:, i * n : (i + 1) * n] = value
                else:
                    outs[per][r // 2, :, i * n : (i + 1) * n] = value.astype(BF16)


def final_kernel(seq, heads, width, parts, shards, len_ref, meta_ref, states_ref, normed_ref, mcot_ref, gain_ref,
                 all0_ref, all1_ref, qkv_ref, wo_ref, wt1_ref, *refs):
    blocks = refs[:parts]
    att_ref, grad_ref, gain_out_ref, wt_s, all_s = refs[parts : parts + 5]
    scratch, sems = refs[parts + 5 : -1], refs[-1]
    n = heads * width
    size = 4 * n // parts
    own = meta_ref[0]

    @pl.when(pl.program_id(0) == 0)
    def _():
        copies = [
            pltpu.make_async_copy(qkv_ref, wt_s.at[own, pl.ds(0, 3 * n)], sems.at[0]),
            pltpu.make_async_copy(wo_ref, wt_s.at[own, pl.ds(3 * n, n)], sems.at[1]),
            pltpu.make_async_copy(wt1_ref, wt_s.at[own ^ 1], sems.at[2]),
        ]
        for k in range(2, shards):
            for r in range(parts):
                place = pl.multiple_of((meta_ref[1] ^ r) * size, 8)
                copies.append(pltpu.make_async_copy(
                    blocks[r].at[k - 2], wt_s.at[own ^ k, pl.ds(place, size)], sems.at[3 + (k - 2) * parts + r]))
        for copy in copies:
            copy.start()
        for copy in copies:
            copy.wait()
        gain_out_ref[...] = jnp.zeros_like(gain_out_ref)

    all_s[own] = all0_ref[...]
    all_s[own ^ 1] = all1_ref[...]
    normed, mcot = normed_ref[...], mcot_ref[...]
    for k in range(2, shards):
        w = [wt_s[own ^ k, i * n : (i + 1) * n] for i in range(4)]
        shard_body(len_ref, normed, mcot, w[0], w[1], w[2], w[3],
                   all_s.at[own ^ k], scratch[4 * (k % 2) : 4 * (k % 2) + 4], seq, heads, width)
    total = None
    grad = None
    for s in range(shards):
        piece = dot_nn(all_s[s, 3], wt_s[s, 3 * n :])
        total = piece if total is None else total + piece
    wide = states_ref[...].astype(F32)
    att_ref[...] = (wide + total).astype(BF16)
    for s in range(shards):
        for i in range(3):
            piece = dot_nn(all_s[s, i], wt_s[s, i * n : (i + 1) * n])
            grad = piece if grad is None else grad + piece
    inv = lax.rsqrt(jnp.mean(wide * wide, axis=-1, keepdims=True) + EPS)
    unit = wide * inv
    gain_out_ref[...] += jnp.sum(grad * unit, axis=0, keepdims=True)
    unit_grad = grad * gain_ref[...]
    corr = jnp.mean(unit_grad * unit, axis=-1, keepdims=True)
    grad_ref[...] = (mcot.astype(F32) + inv * (unit_grad - unit * corr)).astype(BF16)


def body(dp, mp, states, hist_len, norm_gain, qkv_weight, output_weight, cotangent):
    batch, seq, d = states.shape
    _, _, heads, width = qkv_weight.shape
    n = heads * width
    rows = batch * seq
    parts = 8
    low = dp // parts
    i_hi = lax.axis_index("dp") // low
    i_mp = lax.axis_index("mp")
    meta = jnp.stack([i_mp, i_hi]).astype(jnp.int32)

    def hop_dp(x, r):
        return lax.ppermute(x, "dp", [(i, i ^ (r * low)) for i in range(dp)])

    def hop_mp(x, k):
        return lax.ppermute(x, "mp", [(i, i ^ k) for i in range(mp)])

    qkv_rows = jnp.transpose(qkv_weight, (1, 2, 3, 0)).reshape(3 * n, d)
    wo_rows = output_weight.reshape(n, d)
    size = 4 * n // parts
    mine = lax.dynamic_slice_in_dim(jnp.concatenate([qkv_rows, wo_rows], axis=0), i_hi * size, size, 0)

    first = [hop_mp(mine, k) for k in range(1, mp)]

    def spread(block):
        even = {0: block}
        for r in range(2, parts, 2):
            even[r] = hop_dp(block, r)
        blocks = dict(even)
        for r in range(0, parts, 2):
            blocks[r ^ 1] = hop_dp(even[r], 1)
        return [blocks[r] for r in range(parts)]

    near = spread(first[0])
    rest = spread(jnp.stack(first[1:]))

    flat_states = states.reshape(rows, d)
    flat_cot = cotangent.reshape(rows, d)
    gain = norm_gain.reshape(1, d)
    chunk = rows // 4
    grid = rows // chunk
    scratch = [pltpu.VMEM((chunk, n), BF16) for _ in range(4)]
    flops_in = 2 * rows * d * 4 * n
    row_spec = pl.BlockSpec((chunk, d), lambda c, *_: (c, 0))
    all_spec = pl.BlockSpec((4, chunk, n), lambda c, *_: (0, c, 0))
    any_spec = pl.BlockSpec(memory_space=pl.ANY)
    all_shape = jax.ShapeDtypeStruct((4, rows, n), BF16)
    row_shape = jax.ShapeDtypeStruct((rows, d), BF16)

    def whole(shape):
        return pl.BlockSpec(shape, lambda c, *_: tuple(0 for _ in shape))

    def call(kernel, flops, vmem, scalars, steps, in_specs, out_specs, out_shape, scratch_shapes):
        return pl.pallas_call(
            kernel, out_shape=out_shape,
            grid_spec=pltpu.PrefetchScalarGridSpec(
                num_scalar_prefetch=scalars, grid=(steps,), in_specs=in_specs, out_specs=out_specs,
                scratch_shapes=scratch_shapes),
            compiler_params=pltpu.CompilerParams(
                dimension_semantics=("arbitrary",), vmem_limit_bytes=vmem * 1024 * 1024),
            cost_estimate=pl.CostEstimate(flops=flops, bytes_accessed=rows * d * 8, transcendentals=0))

    normed, mcot, all0 = call(
        functools.partial(own_kernel, seq, heads, width), 3 * flops_in, 24, 1, grid,
        [row_spec, row_spec, whole((1, d)), whole((3 * n, d)), whole((n, d))],
        [row_spec, row_spec, all_spec], [row_shape, row_shape, all_shape], scratch,
    )(hist_len, flat_states, flat_cot, gain, qkv_rows, wo_rows)

    piece = (d // parts, 4 * n)
    half = parts // 2
    *kept, sent = call(
        functools.partial(weight_grad_kernel, parts, n), flops_in, 32, 1, 2,
        [pl.BlockSpec((rows, d // 2), lambda c, *_: (0, c))] * 2 + [whole((4, rows, n))],
        [whole(piece)] * half + [whole((half,) + piece)],
        [jax.ShapeDtypeStruct(piece, F32)] * half + [jax.ShapeDtypeStruct((half,) + piece, BF16)],
        [pltpu.VMEM((4, parts, d // parts, n), F32)],
    )(meta, normed, mcot, all0)
    pair = hop_dp(sent, 1)
    kept = [kept[r] + pair[r].astype(F32) for r in range(half)]
    arrived = [hop_dp(kept[r].astype(BF16), 2 * r) for r in range(1, half)]

    all1, wt1 = call(
        functools.partial(far_kernel, seq, heads, width, parts), 3 * flops_in, 24, 2, grid,
        [row_spec, row_spec] + [any_spec] * parts,
        [all_spec, whole((4 * n, d))], [all_shape, jax.ShapeDtypeStruct((4 * n, d), BF16)],
        scratch + [pltpu.SemaphoreType.DMA((parts,))],
    )(hist_len, meta, normed, mcot, *near)

    attended, grad_states, gain_part = call(
        functools.partial(final_kernel, seq, heads, width, parts, mp), 10 * flops_in, 44, 2, grid,
        [row_spec, row_spec, row_spec, whole((1, d)), all_spec, all_spec] + [any_spec] * (3 + parts),
        [row_spec, row_spec, whole((1, d))], [row_shape, row_shape, jax.ShapeDtypeStruct((1, d), F32)],
        [pltpu.VMEM((mp, 4 * n, d), BF16), pltpu.VMEM((mp, 4, chunk, n), BF16)] + scratch * 2
        + [pltpu.SemaphoreType.DMA((3 + (mp - 2) * parts,))],
    )(hist_len, meta, flat_states, normed, mcot, gain, all0, all1, qkv_rows, wo_rows, wt1, *rest)

    summed = kept[0]
    for part in arrived:
        summed = summed + part.astype(F32)
    gain_sum = gain_part
    for r in range(1, parts):
        gain_sum = gain_sum + hop_dp(gain_part, r)
    gain_piece = lax.dynamic_slice_in_dim(gain_sum.reshape(d), i_hi * (d // parts), d // parts, 0)
    if low > 1:
        groups = [[hi * low + lo for lo in range(low)] for hi in range(parts)]
        summed = lax.psum_scatter(summed, "dp", scatter_dimension=0, axis_index_groups=groups, tiled=True)
        gain_piece = lax.psum_scatter(gain_piece, "dp", scatter_dimension=0, axis_index_groups=groups, tiled=True)
    across = summed.T
    grad_qkv = jnp.transpose(across[: 3 * n].reshape(3, heads, width, -1), (3, 0, 1, 2))
    grad_output = across[3 * n :].reshape(heads, width, -1)
    return (attended.reshape(batch, seq, d), grad_states.reshape(batch, seq, d), grad_qkv, grad_output, gain_piece)


def solution(mesh):
    placed = (
        P("dp", None, None),
        P("dp"),
        P(),
        P(None, None, "mp", None),
        P("mp", None, None),
        P("dp", None, None),
    )
    return jax.shard_map(
        functools.partial(body, mesh.shape["dp"], mesh.shape["mp"]),
        mesh=mesh,
        in_specs=placed,
        out_specs=(
            P("dp", None, None),
            P("dp", None, None),
            P("dp", None, "mp", None),
            P("mp", None, "dp"),
            P("dp"),
        ),
        check_vma=False,
    )
```

```python
import functools

import jax
import jax.numpy as jnp
from jax import lax
from jax.experimental import pallas as pl
from jax.experimental.pallas import tpu as pltpu
from jax.sharding import PartitionSpec as P


LEVELS = 4
EPS = 1e-06
F32 = jnp.float32
BF16 = jnp.bfloat16


def dot_nt(a, b):
    return lax.dot_general(a, b, (((1,), (1,)), ((), ())), preferred_element_type=F32)


def dot_nn(a, b):
    return lax.dot_general(a, b, (((1,), (0,)), ((), ())), preferred_element_type=F32)


def dot_tn(a, b):
    return lax.dot_general(a, b, (((0,), (0,)), ((), ())), preferred_element_type=F32)


def attention(refs, out_ref, valid, heads, width):
    q_s, k_s, v_s, g_s = refs
    count = len(valid)
    seq = q_s.shape[0] // count
    lane_head = lax.broadcasted_iota(jnp.int32, (1, heads * width), 1) // width
    masks = [(lane_head == h).astype(BF16) for h in range(heads)]
    rows = [slice(b * seq, (b + 1) * seq) for b in range(count)]

    def blocks(x):
        return jnp.concatenate([x * m for m in masks], axis=0)

    def diagonal(full):
        out = full[:seq]
        for h in range(1, heads):
            out = jnp.where(lane_head == h, full[h * seq : (h + 1) * seq], out)
        return out

    scores = [dot_nt(k_s[r], blocks(q_s[r])) for r in rows]
    grad_prob = [dot_nt(v_s[r], blocks(g_s[r])) for r in rows]
    probs, grad_scores = [], []
    for score, grad, length in zip(scores, grad_prob, valid):
        row = lax.broadcasted_iota(jnp.int32, score.shape, 0)
        score = jnp.where(row < length, score, -1e30)
        exp_score = jnp.exp(score - jnp.max(score, axis=0, keepdims=True))
        prob = exp_score * (1.0 / jnp.sum(exp_score, axis=0, keepdims=True))
        probs.append(prob.astype(BF16))
        delta = jnp.sum(prob * grad, axis=0, keepdims=True)
        grad_scores.append((prob * (grad - delta)).astype(BF16))
    for r, prob, grad_score in zip(rows, probs, grad_scores):
        out_ref[2, r] = dot_nn(prob, blocks(g_s[r])).astype(BF16)
        out_ref[1, r] = dot_nn(grad_score, blocks(q_s[r])).astype(BF16)
        out_ref[3, r] = diagonal(dot_tn(prob, v_s[r])).astype(BF16)
        out_ref[0, r] = diagonal(dot_tn(grad_score, k_s[r])).astype(BF16)


def keep_rows(len_ref, first, count, seq):
    rows = [lax.broadcasted_iota(jnp.int32, (seq, 1), 0) < LEVELS * len_ref[first + b] for b in range(count)]
    return jnp.concatenate([r.astype(F32) for r in rows], axis=0)


def shard_body(len_ref, normed, mcot, w_q, w_k, w_v, w_o, out_ref, scratch, seq, heads, width):
    q_s, k_s, v_s, g_s = scratch
    chunk = pl.program_id(0)
    count = normed.shape[0] // seq
    q_s[...] = dot_nt(normed, w_q).astype(BF16)
    k_s[...] = dot_nt(normed, w_k).astype(BF16)
    v_s[...] = dot_nt(normed, w_v).astype(BF16)
    g_s[...] = dot_nt(mcot, w_o).astype(BF16)
    attention(scratch, out_ref, [LEVELS * len_ref[chunk * count + b] for b in range(count)], heads, width)


def own_kernel(seq, heads, width, len_ref, states_ref, cot_ref, gain_ref, qkv_ref, wo_ref,
               normed_ref, mcot_ref, out_ref, *scratch):
    wide = states_ref[...].astype(F32)
    inv = lax.rsqrt(jnp.mean(wide * wide, axis=-1, keepdims=True) + EPS)
    normed = (wide * inv * gain_ref[...]).astype(BF16)
    normed_ref[...] = normed
    count = normed.shape[0] // seq
    keep = keep_rows(len_ref, pl.program_id(0) * count, count, seq)
    mcot = (cot_ref[...].astype(F32) * keep).astype(BF16)
    mcot_ref[...] = mcot
    n = heads * width
    shard_body(len_ref, normed, mcot, qkv_ref[:n], qkv_ref[n : 2 * n], qkv_ref[2 * n : 3 * n], wo_ref[...],
               out_ref.at[:], scratch, seq, heads, width)


def far_kernel(seq, heads, width, len_ref, meta_ref, normed_ref, mcot_ref, *refs):
    blocks = refs[:4]
    out_ref, wt_ref, q_s, k_s, v_s, g_s, sems = refs[4:]
    n = heads * width

    @pl.when(pl.program_id(0) == 0)
    def _():
        copies = []
        for r in range(4):
            place = pl.multiple_of(((meta_ref[1] % 4) ^ r) * n, 8)
            copies.append(pltpu.make_async_copy(blocks[r], wt_ref.at[pl.ds(place, n)], sems.at[r]))
        for copy in copies:
            copy.start()
        for copy in copies:
            copy.wait()

    w = [wt_ref[i * n : (i + 1) * n] for i in range(4)]
    shard_body(len_ref, normed_ref[...], mcot_ref[...], w[0], w[1], w[2], w[3],
               out_ref.at[:], (q_s, k_s, v_s, g_s), seq, heads, width)


def weight_grad_kernel(parts, n, meta_ref, normed_ref, mcot_ref, all_ref, *refs):
    outs, acc = refs[:-1], refs[-1]
    step = pl.program_id(0)
    rows = normed_ref.shape[1]
    size = rows * pl.num_programs(0) // parts
    per = parts // 2
    for i in range(4):
        left = mcot_ref[...] if i == 3 else normed_ref[...]
        piece = dot_tn(left, all_ref[i])
        for c in range(per):
            acc[i, step * per + c] = piece[c * size : (c + 1) * size]

    @pl.when(step == pl.num_programs(0) - 1)
    def _():
        for r in range(parts):
            for i in range(4):
                value = acc[i, meta_ref[1] ^ r]
                if r % 2 == 0:
                    outs[r // 2][:, i * n : (i + 1) * n] = value
                else:
                    outs[per][r // 2, :, i * n : (i + 1) * n] = value.astype(BF16)


def final_kernel(seq, heads, width, parts, shards, len_ref, meta_ref, states_ref, normed_ref, mcot_ref, gain_ref,
                 all0_ref, all1_ref, qkv_ref, wo_ref, wt1_ref, *refs):
    blocks = refs[:parts]
    att_ref, grad_ref, gain_out_ref, wt_s, all_s = refs[parts : parts + 5]
    scratch, sems = refs[parts + 5 : -1], refs[-1]
    n = heads * width
    size = 4 * n // parts
    own = meta_ref[0]

    @pl.when(pl.program_id(0) == 0)
    def _():
        copies = [
            pltpu.make_async_copy(qkv_ref, wt_s.at[own, pl.ds(0, 3 * n)], sems.at[0]),
            pltpu.make_async_copy(wo_ref, wt_s.at[own, pl.ds(3 * n, n)], sems.at[1]),
            pltpu.make_async_copy(wt1_ref, wt_s.at[own ^ 1], sems.at[2]),
        ]
        for k in range(2, shards):
            for r in range(parts):
                place = pl.multiple_of((meta_ref[1] ^ r) * size, 8)
                copies.append(pltpu.make_async_copy(
                    blocks[r].at[k - 2], wt_s.at[own ^ k, pl.ds(place, size)], sems.at[3 + (k - 2) * parts + r]))
        for copy in copies:
            copy.start()
        for copy in copies:
            copy.wait()
        gain_out_ref[...] = jnp.zeros_like(gain_out_ref)

    all_s[own] = all0_ref[...]
    all_s[own ^ 1] = all1_ref[...]
    normed, mcot = normed_ref[...], mcot_ref[...]
    for k in range(2, shards):
        w = [wt_s[own ^ k, i * n : (i + 1) * n] for i in range(4)]
        shard_body(len_ref, normed, mcot, w[0], w[1], w[2], w[3],
                   all_s.at[own ^ k], scratch[4 * (k % 2) : 4 * (k % 2) + 4], seq, heads, width)

    def chain(kinds, rows, columns):
        out = None
        for s in range(shards):
            for i in kinds:
                piece = dot_nn(all_s[s, i, rows], wt_s[s, i * n : (i + 1) * n, columns])
                out = piece if out is None else out + piece
        return out

    def project(kinds):
        count, d = states_ref.shape
        cut, half = d - 256, count // 2
        last = [chain(kinds, slice(p * half, (p + 1) * half), slice(cut, d)) for p in range(2)]
        return jnp.concatenate([chain(kinds, slice(None), slice(0, cut)), jnp.concatenate(last, axis=0)], axis=1)

    total = project((3,))
    grad = project((0, 1, 2))
    wide = states_ref[...].astype(F32)
    att_ref[...] = (wide + total).astype(BF16)
    inv = lax.rsqrt(jnp.mean(wide * wide, axis=-1, keepdims=True) + EPS)
    unit = wide * inv
    gain_out_ref[...] += jnp.sum(grad * unit, axis=0, keepdims=True)
    unit_grad = grad * gain_ref[...]
    corr = jnp.mean(unit_grad * unit, axis=-1, keepdims=True)
    grad_ref[...] = (mcot.astype(F32) + inv * (unit_grad - unit * corr)).astype(BF16)


def body(dp, mp, states, hist_len, norm_gain, qkv_weight, output_weight, cotangent):
    batch, seq, d = states.shape
    _, _, heads, width = qkv_weight.shape
    n = heads * width
    rows = batch * seq
    parts = 8
    low = dp // parts
    i_hi = lax.axis_index("dp") // low
    i_mp = lax.axis_index("mp")
    meta = jnp.stack([i_mp, i_hi]).astype(jnp.int32)

    def hop_dp(x, r):
        return lax.ppermute(x, "dp", [(i, i ^ (r * low)) for i in range(dp)])

    def hop_mp(x, k):
        return lax.ppermute(x, "mp", [(i, i ^ k) for i in range(mp)])

    qkv_rows = jnp.transpose(qkv_weight, (1, 2, 3, 0)).reshape(3 * n, d)
    wo_rows = output_weight.reshape(n, d)
    size = 4 * n // parts
    stacked = jnp.concatenate([qkv_rows, wo_rows], axis=0)
    mine = lax.dynamic_slice_in_dim(stacked, i_hi * size, size, 0)
    mine_near = lax.dynamic_slice_in_dim(stacked, (i_hi % 4) * n, n, 0)

    near = [hop_mp(mine_near, 1)]
    first = [hop_mp(mine, k) for k in range(2, mp)]
    across = hop_dp(near[0], 2)
    near = [near[0], hop_dp(near[0], 1), across, hop_dp(across, 1)]
    even = {0: jnp.stack(first)}
    for r in range(2, parts, 2):
        even[r] = hop_dp(even[0], r)
    blocks = dict(even)
    blocks[1] = hop_dp(even[0], 1)
    for r in range(2, parts, 2):
        blocks[r ^ 1] = hop_dp(even[r], 1)
    rest = [blocks[r] for r in range(parts)]

    flat_states = states.reshape(rows, d)
    flat_cot = cotangent.reshape(rows, d)
    gain = norm_gain.reshape(1, d)
    chunk = rows // 4
    grid = rows // chunk
    scratch = [pltpu.VMEM((chunk, n), BF16) for _ in range(8)]
    big_scratch = [pltpu.VMEM((rows // 2, n), BF16) for _ in range(4)]
    flops_in = 2 * rows * d * 4 * n
    big = rows // 2

    def row_of(size):
        return pl.BlockSpec((size, d), lambda c, *_: (c, 0))

    def all_of(size):
        return pl.BlockSpec((4, size, n), lambda c, *_: (0, c, 0))

    any_spec = pl.BlockSpec(memory_space=pl.ANY)
    all_shape = jax.ShapeDtypeStruct((4, rows, n), BF16)
    row_shape = jax.ShapeDtypeStruct((rows, d), BF16)

    def in_hbm(x):
        return pltpu.with_memory_space_constraint(x, pltpu.HBM)

    def whole(shape):
        return pl.BlockSpec(shape, lambda c, *_: tuple(0 for _ in shape))

    def call(kernel, flops, vmem, scalars, steps, in_specs, out_specs, out_shape, scratch_shapes):
        return pl.pallas_call(
            kernel, out_shape=out_shape,
            grid_spec=pltpu.PrefetchScalarGridSpec(
                num_scalar_prefetch=scalars, grid=(steps,), in_specs=in_specs, out_specs=out_specs,
                scratch_shapes=scratch_shapes),
            compiler_params=pltpu.CompilerParams(
                dimension_semantics=("arbitrary",), vmem_limit_bytes=vmem * 1024 * 1024),
            cost_estimate=pl.CostEstimate(flops=flops, bytes_accessed=rows * d * 8, transcendentals=0))

    normed, mcot, all0 = call(
        functools.partial(own_kernel, seq, heads, width), 3 * flops_in, 28, 1, 2,
        [row_of(big)] * 2 + [whole((1, d)), whole((3 * n, d)), whole((n, d))],
        [row_of(big)] * 2 + [all_of(big)], [row_shape, row_shape, all_shape], big_scratch,
    )(hist_len, in_hbm(flat_states), in_hbm(flat_cot), gain, in_hbm(qkv_rows), in_hbm(wo_rows))

    piece = (d // parts, 4 * n)
    half = parts // 2
    *kept, sent = call(
        functools.partial(weight_grad_kernel, parts, n), flops_in, 32, 1, 2,
        [pl.BlockSpec((rows, d // 2), lambda c, *_: (0, c))] * 2 + [whole((4, rows, n))],
        [whole(piece)] * half + [whole((half,) + piece)],
        [jax.ShapeDtypeStruct(piece, F32)] * half + [jax.ShapeDtypeStruct((half,) + piece, BF16)],
        [pltpu.VMEM((4, parts, d // parts, n), F32)],
    )(meta, normed, mcot, all0)
    pair = hop_dp(sent, 1)
    kept = [kept[r] + pair[r].astype(F32) for r in range(half)]
    arrived = [hop_dp(kept[r].astype(BF16), 2 * r) for r in range(1, half)]

    all1, wt1 = call(
        functools.partial(far_kernel, seq, heads, width), 3 * flops_in, 28, 2, 2,
        [row_of(big)] * 2 + [any_spec] * 4,
        [all_of(big), whole((4 * n, d))], [all_shape, jax.ShapeDtypeStruct((4 * n, d), BF16)],
        big_scratch + [pltpu.SemaphoreType.DMA((4,))],
    )(hist_len, meta, normed, mcot, *near)

    attended, grad_states, gain_part = call(
        functools.partial(final_kernel, seq, heads, width, parts, mp), 10 * flops_in, 30, 2, grid,
        [row_of(chunk)] * 3 + [whole((1, d)), all_of(chunk), all_of(chunk)] + [any_spec] * (3 + parts),
        [row_of(chunk)] * 2 + [whole((1, d))], [row_shape, row_shape, jax.ShapeDtypeStruct((1, d), F32)],
        [pltpu.VMEM((mp, 4 * n, d), BF16), pltpu.VMEM((mp, 4, chunk, n), BF16)] + scratch
        + [pltpu.SemaphoreType.DMA((3 + (mp - 2) * parts,))],
    )(hist_len, meta, flat_states, normed, mcot, gain, all0, all1, qkv_rows, wo_rows, wt1, *rest)

    summed = kept[0]
    for part in arrived:
        summed = summed + part.astype(F32)
    gain_pair = gain_part + hop_dp(gain_part, 1)
    gain_sum = gain_pair
    for r in range(2, parts, 2):
        gain_sum = gain_sum + hop_dp(gain_pair, r)
    gain_piece = lax.dynamic_slice_in_dim(gain_sum.reshape(d), i_hi * (d // parts), d // parts, 0)
    if low > 1:
        groups = [[hi * low + lo for lo in range(low)] for hi in range(parts)]
        summed = lax.psum_scatter(summed, "dp", scatter_dimension=0, axis_index_groups=groups, tiled=True)
        gain_piece = lax.psum_scatter(gain_piece, "dp", scatter_dimension=0, axis_index_groups=groups, tiled=True)
    across = summed.T
    grad_qkv = jnp.transpose(across[: 3 * n].reshape(3, heads, width, -1), (3, 0, 1, 2))
    grad_output = across[3 * n :].reshape(heads, width, -1)
    return (attended.reshape(batch, seq, d), grad_states.reshape(batch, seq, d), grad_qkv, grad_output, gain_piece)


def solution(mesh):
    placed = (
        P("dp", None, None),
        P("dp"),
        P(),
        P(None, None, "mp", None),
        P("mp", None, None),
        P("dp", None, None),
    )
    return jax.shard_map(
        functools.partial(body, mesh.shape["dp"], mesh.shape["mp"]),
        mesh=mesh,
        in_specs=placed,
        out_specs=(
            P("dp", None, None),
            P("dp", None, None),
            P("dp", None, "mp", None),
            P("mp", None, "dp"),
            P("dp"),
        ),
        check_vma=False,
    )
```

```python
import functools

import jax
import jax.numpy as jnp
from jax import lax
from jax.experimental import pallas as pl
from jax.experimental.pallas import tpu as pltpu
from jax.sharding import PartitionSpec as P


LEVELS = 4
EPS = 1e-06
F32 = jnp.float32
BF16 = jnp.bfloat16


def dot_nt(a, b):
    return lax.dot_general(a, b, (((1,), (1,)), ((), ())), preferred_element_type=F32)


def dot_nn(a, b):
    return lax.dot_general(a, b, (((1,), (0,)), ((), ())), preferred_element_type=F32)


def dot_tn(a, b):
    return lax.dot_general(a, b, (((0,), (0,)), ((), ())), preferred_element_type=F32)


def project(pairs):
    def chain(rows, columns):
        out = None
        for left, right in pairs:
            part = dot_nn(left[rows], right[:, columns])
            out = part if out is None else out + part
        return out

    count, d = pairs[0][0].shape[0], pairs[0][1].shape[1]
    cut, half = d - 256, count // 2
    last = [chain(slice(p * half, (p + 1) * half), slice(cut, d)) for p in range(2)]
    return jnp.concatenate([chain(slice(None), slice(0, cut)), jnp.concatenate(last, axis=0)], axis=1)


def attention(refs, out_ref, valid, heads, width):
    q_s, k_s, v_s, g_s = refs
    count = len(valid)
    seq = q_s.shape[0] // count
    lane_head = lax.broadcasted_iota(jnp.int32, (1, heads * width), 1) // width
    masks = [(lane_head == h).astype(BF16) for h in range(heads)]
    rows = [slice(b * seq, (b + 1) * seq) for b in range(count)]

    def blocks(x):
        return jnp.concatenate([x * m for m in masks], axis=0)

    def diagonal(full):
        out = full[:seq]
        for h in range(1, heads):
            out = jnp.where(lane_head == h, full[h * seq : (h + 1) * seq], out)
        return out

    scores = [dot_nt(k_s[r], blocks(q_s[r])) for r in rows]
    grad_prob = [dot_nt(v_s[r], blocks(g_s[r])) for r in rows]
    probs, grad_scores = [], []
    for score, grad, length in zip(scores, grad_prob, valid):
        row = lax.broadcasted_iota(jnp.int32, score.shape, 0)
        score = jnp.where(row < length, score, -1e30)
        exp_score = jnp.exp(score - jnp.max(score, axis=0, keepdims=True))
        prob = exp_score * (1.0 / jnp.sum(exp_score, axis=0, keepdims=True))
        probs.append(prob.astype(BF16))
        delta = jnp.sum(prob * grad, axis=0, keepdims=True)
        grad_scores.append((prob * (grad - delta)).astype(BF16))
    for r, prob, grad_score in zip(rows, probs, grad_scores):
        out_ref[2, r] = dot_nn(prob, blocks(g_s[r])).astype(BF16)
        out_ref[1, r] = dot_nn(grad_score, blocks(q_s[r])).astype(BF16)
        out_ref[3, r] = diagonal(dot_tn(prob, v_s[r])).astype(BF16)
        out_ref[0, r] = diagonal(dot_tn(grad_score, k_s[r])).astype(BF16)


def keep_rows(len_ref, first, count, seq):
    rows = [lax.broadcasted_iota(jnp.int32, (seq, 1), 0) < LEVELS * len_ref[first + b] for b in range(count)]
    return jnp.concatenate([r.astype(F32) for r in rows], axis=0)


def shard_body(len_ref, normed, mcot, w_q, w_k, w_v, w_o, out_ref, scratch, seq, heads, width):
    q_s, k_s, v_s, g_s = scratch
    chunk = pl.program_id(0)
    count = normed.shape[0] // seq
    q_s[...] = dot_nt(normed, w_q).astype(BF16)
    k_s[...] = dot_nt(normed, w_k).astype(BF16)
    v_s[...] = dot_nt(normed, w_v).astype(BF16)
    g_s[...] = dot_nt(mcot, w_o).astype(BF16)
    attention(scratch, out_ref, [LEVELS * len_ref[chunk * count + b] for b in range(count)], heads, width)


def own_kernel(seq, heads, width, len_ref, states_ref, cot_ref, gain_ref, qkv_ref, wo_ref,
               normed_ref, mcot_ref, out_ref, gain_out_ref, *scratch):
    wide = states_ref[...].astype(F32)
    inv = lax.rsqrt(jnp.mean(wide * wide, axis=-1, keepdims=True) + EPS)
    normed = (wide * inv * gain_ref[...]).astype(BF16)
    normed_ref[...] = normed
    count = normed.shape[0] // seq
    keep = keep_rows(len_ref, pl.program_id(0) * count, count, seq)
    mcot = (cot_ref[...].astype(F32) * keep).astype(BF16)
    mcot_ref[...] = mcot
    n = heads * width
    shard_body(len_ref, normed, mcot, qkv_ref[:n], qkv_ref[n : 2 * n], qkv_ref[2 * n : 3 * n], wo_ref[...],
               out_ref.at[:], scratch, seq, heads, width)

    @pl.when(pl.program_id(0) == 0)
    def _():
        gain_out_ref[...] = jnp.zeros_like(gain_out_ref)

    grad = project([(out_ref.at[i], qkv_ref.at[i * n : (i + 1) * n]) for i in range(3)])
    gain_out_ref[...] += jnp.sum(grad * (states_ref[...].astype(F32) * inv), axis=0, keepdims=True)


def far_kernel(seq, heads, width, len_ref, meta_ref, normed_ref, mcot_ref, *refs):
    blocks = refs[:2]
    out_ref, wt_ref, q_s, k_s, v_s, g_s, sems = refs[2:]
    n = heads * width

    @pl.when(pl.program_id(0) == 0)
    def _():
        copies = []
        for r in range(2):
            place = pl.multiple_of(((meta_ref[1] % 2) ^ r) * 2 * n, 8)
            copies.append(pltpu.make_async_copy(blocks[r], wt_ref.at[pl.ds(place, 2 * n)], sems.at[r]))
        for copy in copies:
            copy.start()
        for copy in copies:
            copy.wait()

    w = [wt_ref[i * n : (i + 1) * n] for i in range(4)]
    shard_body(len_ref, normed_ref[...], mcot_ref[...], w[0], w[1], w[2], w[3],
               out_ref.at[:], (q_s, k_s, v_s, g_s), seq, heads, width)


def weight_grad_kernel(parts, n, meta_ref, normed_ref, mcot_ref, all_ref, *refs):
    outs, acc = refs[:-1], refs[-1]
    step = pl.program_id(0)
    rows = normed_ref.shape[1]
    size = rows * pl.num_programs(0) // parts
    per = parts // 2
    for i in range(4):
        left = mcot_ref[...] if i == 3 else normed_ref[...]
        piece = dot_tn(left, all_ref[i])
        for c in range(per):
            acc[i, step * per + c] = piece[c * size : (c + 1) * size]

    @pl.when(step == pl.num_programs(0) - 1)
    def _():
        for r in range(parts):
            for i in range(4):
                value = acc[i, meta_ref[1] ^ r]
                if r % 2 == 0:
                    outs[r // 2][:, i * n : (i + 1) * n] = value
                else:
                    outs[per][r // 2, :, i * n : (i + 1) * n] = value.astype(BF16)


def final_kernel(seq, heads, width, parts, shards, len_ref, meta_ref, states_ref, normed_ref, mcot_ref, gain_ref,
                 all0_ref, all1_ref, qkv_ref, wo_ref, wt1_ref, *refs):
    blocks = refs[:parts]
    att_ref, grad_ref, wt_s, all_s = refs[parts : parts + 4]
    scratch, sems = refs[parts + 4 : -1], refs[-1]
    n = heads * width
    size = 4 * n // parts
    own = meta_ref[0]

    @pl.when(pl.program_id(0) == 0)
    def _():
        copies = [
            pltpu.make_async_copy(qkv_ref, wt_s.at[own, pl.ds(0, 3 * n)], sems.at[0]),
            pltpu.make_async_copy(wo_ref, wt_s.at[own, pl.ds(3 * n, n)], sems.at[1]),
            pltpu.make_async_copy(wt1_ref, wt_s.at[own ^ 1], sems.at[2]),
        ]
        for k in range(2, shards):
            for r in range(parts):
                place = pl.multiple_of((meta_ref[1] ^ r) * size, 8)
                copies.append(pltpu.make_async_copy(
                    blocks[r].at[k - 2], wt_s.at[own ^ k, pl.ds(place, size)], sems.at[3 + (k - 2) * parts + r]))
        for copy in copies:
            copy.start()
        for copy in copies:
            copy.wait()

    all_s[own] = all0_ref[...]
    all_s[own ^ 1] = all1_ref[...]
    normed, mcot = normed_ref[...], mcot_ref[...]
    count = normed.shape[0] // seq
    valid = [LEVELS * len_ref[pl.program_id(0) * count + b] for b in range(count)]
    for k in range(2, shards):
        for i in range(4):
            left = mcot if i == 3 else normed
            scratch[4 * (k % 2) + i][...] = dot_nt(left, wt_s[own ^ k, i * n : (i + 1) * n]).astype(BF16)
    for k in range(2, shards):
        attention(scratch[4 * (k % 2) : 4 * (k % 2) + 4], all_s.at[own ^ k], valid, heads, width)

    def piece(kind, shard):
        return all_s.at[shard, kind], wt_s.at[shard, kind * n : (kind + 1) * n]

    total = project([piece(3, s) for s in range(shards)])
    grad = project([piece(i, s) for s in range(shards) for i in range(3)])
    wide = states_ref[...].astype(F32)
    att_ref[...] = (wide + total).astype(BF16)
    inv = lax.rsqrt(jnp.mean(wide * wide, axis=-1, keepdims=True) + EPS)
    unit = wide * inv
    unit_grad = grad * gain_ref[...]
    corr = jnp.mean(unit_grad * unit, axis=-1, keepdims=True)
    grad_ref[...] = (mcot.astype(F32) + inv * (unit_grad - unit * corr)).astype(BF16)


def body(dp, mp, states, hist_len, norm_gain, qkv_weight, output_weight, cotangent):
    batch, seq, d = states.shape
    _, _, heads, width = qkv_weight.shape
    n = heads * width
    rows = batch * seq
    parts = 8
    low = dp // parts
    i_hi = lax.axis_index("dp") // low
    i_mp = lax.axis_index("mp")
    meta = jnp.stack([i_mp, i_hi]).astype(jnp.int32)

    def hop_dp(x, r):
        return lax.ppermute(x, "dp", [(i, i ^ (r * low)) for i in range(dp)])

    def hop_mp(x, k):
        return lax.ppermute(x, "mp", [(i, i ^ k) for i in range(mp)])

    qkv_rows = jnp.transpose(qkv_weight, (1, 2, 3, 0)).reshape(3 * n, d)
    wo_rows = output_weight.reshape(n, d)
    size = 4 * n // parts
    stacked = jnp.concatenate([qkv_rows, wo_rows], axis=0)
    mine = lax.dynamic_slice_in_dim(stacked, i_hi * size, size, 0)
    mine_near = lax.dynamic_slice_in_dim(stacked, (i_hi % 2) * 2 * n, 2 * n, 0)

    near = [hop_mp(mine_near, 1)]
    first = [hop_mp(mine, k) for k in range(2, mp)]
    near.append(hop_dp(near[0], 1))
    even = {0: jnp.stack(first)}
    for r in range(2, parts, 2):
        even[r] = hop_dp(even[0], r)
    blocks = dict(even)
    blocks[1] = hop_dp(even[0], 1)
    for r in range(2, parts, 2):
        blocks[r ^ 1] = hop_dp(even[r], 1)
    rest = [blocks[r] for r in range(parts)]

    flat_states = states.reshape(rows, d)
    flat_cot = cotangent.reshape(rows, d)
    gain = norm_gain.reshape(1, d)
    chunk = rows // 4
    grid = rows // chunk
    scratch = [pltpu.VMEM((chunk, n), BF16) for _ in range(8)]
    big_scratch = [pltpu.VMEM((rows // 2, n), BF16) for _ in range(4)]
    flops_in = 2 * rows * d * 4 * n
    big = rows // 2

    def row_of(size):
        return pl.BlockSpec((size, d), lambda c, *_: (c, 0))

    def all_of(size):
        return pl.BlockSpec((4, size, n), lambda c, *_: (0, c, 0))

    any_spec = pl.BlockSpec(memory_space=pl.ANY)
    all_shape = jax.ShapeDtypeStruct((4, rows, n), BF16)
    row_shape = jax.ShapeDtypeStruct((rows, d), BF16)

    def in_hbm(x):
        return pltpu.with_memory_space_constraint(x, pltpu.HBM)

    def whole(shape):
        return pl.BlockSpec(shape, lambda c, *_: tuple(0 for _ in shape))

    def call(kernel, flops, vmem, scalars, steps, in_specs, out_specs, out_shape, scratch_shapes):
        return pl.pallas_call(
            kernel, out_shape=out_shape,
            grid_spec=pltpu.PrefetchScalarGridSpec(
                num_scalar_prefetch=scalars, grid=(steps,), in_specs=in_specs, out_specs=out_specs,
                scratch_shapes=scratch_shapes),
            compiler_params=pltpu.CompilerParams(
                dimension_semantics=("arbitrary",), vmem_limit_bytes=vmem * 1024 * 1024),
            cost_estimate=pl.CostEstimate(flops=flops, bytes_accessed=rows * d * 8, transcendentals=0))

    normed, mcot, all0, gain_part = call(
        functools.partial(own_kernel, seq, heads, width), 3 * flops_in, 28, 1, 2,
        [row_of(big)] * 2 + [whole((1, d)), whole((3 * n, d)), whole((n, d))],
        [row_of(big)] * 2 + [all_of(big), whole((1, d))],
        [row_shape, row_shape, all_shape, jax.ShapeDtypeStruct((1, d), F32)], big_scratch,
    )(hist_len, in_hbm(flat_states), in_hbm(flat_cot), gain, in_hbm(qkv_rows), in_hbm(wo_rows))

    piece = (d // parts, 4 * n)
    half = parts // 2
    *kept, sent = call(
        functools.partial(weight_grad_kernel, parts, n), flops_in, 32, 1, 2,
        [pl.BlockSpec((rows, d // 2), lambda c, *_: (0, c))] * 2 + [whole((4, rows, n))],
        [whole(piece)] * half + [whole((half,) + piece)],
        [jax.ShapeDtypeStruct(piece, F32)] * half + [jax.ShapeDtypeStruct((half,) + piece, BF16)],
        [pltpu.VMEM((4, parts, d // parts, n), F32)],
    )(meta, normed, mcot, all0)
    others = [hop_mp(gain_part, k) for k in range(1, mp)]
    all1, wt1 = call(
        functools.partial(far_kernel, seq, heads, width), 3 * flops_in, 28, 2, 2,
        [row_of(big)] * 2 + [any_spec] * 2,
        [all_of(big), whole((4 * n, d))], [all_shape, jax.ShapeDtypeStruct((4 * n, d), BF16)],
        big_scratch + [pltpu.SemaphoreType.DMA((2,))],
    )(hist_len, meta, normed, mcot, *near)

    all1, others = lax.optimization_barrier((all1, others))
    level = [gain_part] + others
    while len(level) > 1:
        level = [level[i] + level[i + 1] for i in range(0, len(level), 2)]
    gain_part = level[0]
    pair = hop_dp(sent, 1)
    gain_part = gain_part + hop_dp(gain_part, 1)
    kept = [kept[r] + pair[r].astype(F32) for r in range(half)]
    rounded = lax.reduce_precision(gain_part, 8, 7)
    tail = jnp.concatenate([rounded, gain_part - rounded, jnp.zeros((14, d), F32)], axis=0).astype(BF16)
    arrived = [
        hop_dp(jnp.concatenate([kept[r].astype(BF16), tail], axis=0), 2 * r) for r in range(1, half)
    ]

    attended, grad_states = call(
        functools.partial(final_kernel, seq, heads, width, parts, mp), 10 * flops_in, 30, 2, grid,
        [row_of(chunk)] * 3 + [whole((1, d)), all_of(chunk), all_of(chunk)] + [any_spec] * (3 + parts),
        [row_of(chunk)] * 2, [row_shape, row_shape],
        [pltpu.VMEM((mp, 4 * n, d), BF16), pltpu.VMEM((mp, 4, chunk, n), BF16)] + scratch
        + [pltpu.SemaphoreType.DMA((3 + (mp - 2) * parts,))],
    )(hist_len, meta, flat_states, normed, mcot, gain, all0, all1, qkv_rows, wo_rows, wt1, *rest)

    attended, arrived = lax.optimization_barrier((attended, arrived))
    summed, gain_sum = kept[0], gain_part
    for part in arrived:
        summed = summed + part[: d // parts].astype(F32)
        gain_sum = gain_sum + (part[d // parts].astype(F32) + part[d // parts + 1].astype(F32))
    gain_piece = lax.dynamic_slice_in_dim(gain_sum.reshape(d), i_hi * (d // parts), d // parts, 0)
    if low > 1:
        groups = [[hi * low + lo for lo in range(low)] for hi in range(parts)]
        summed = lax.psum_scatter(summed, "dp", scatter_dimension=0, axis_index_groups=groups, tiled=True)
        gain_piece = lax.psum_scatter(gain_piece, "dp", scatter_dimension=0, axis_index_groups=groups, tiled=True)
    across = summed.T
    grad_qkv = jnp.transpose(across[: 3 * n].reshape(3, heads, width, -1), (3, 0, 1, 2))
    grad_output = across[3 * n :].reshape(heads, width, -1)
    return (attended.reshape(batch, seq, d), grad_states.reshape(batch, seq, d), grad_qkv, grad_output, gain_piece)


def solution(mesh):
    placed = (
        P("dp", None, None),
        P("dp"),
        P(),
        P(None, None, "mp", None),
        P("mp", None, None),
        P("dp", None, None),
    )
    return jax.shard_map(
        functools.partial(body, mesh.shape["dp"], mesh.shape["mp"]),
        mesh=mesh,
        in_specs=placed,
        out_specs=(
            P("dp", None, None),
            P("dp", None, None),
            P("dp", None, "mp", None),
            P("mp", None, "dp"),
            P("dp"),
        ),
        check_vma=False,
    )
```

```python
import functools

import jax
import jax.numpy as jnp
from jax import lax
from jax.experimental import pallas as pl
from jax.experimental.pallas import tpu as pltpu
from jax.sharding import PartitionSpec as P


LEVELS = 4
EPS = 1e-06
F32 = jnp.float32
BF16 = jnp.bfloat16


def dot_nt(a, b):
    return lax.dot_general(a, b, (((1,), (1,)), ((), ())), preferred_element_type=F32)


def dot_nn(a, b):
    return lax.dot_general(a, b, (((1,), (0,)), ((), ())), preferred_element_type=F32)


def dot_tn(a, b):
    return lax.dot_general(a, b, (((0,), (0,)), ((), ())), preferred_element_type=F32)


def project(pairs):
    def chain(rows, columns):
        out = None
        for left, right in pairs:
            part = dot_nn(left[rows], right[:, columns])
            out = part if out is None else out + part
        return out

    count, d = pairs[0][0].shape[0], pairs[0][1].shape[1]
    cut, half = d - 256, count // 2
    last = [chain(slice(p * half, (p + 1) * half), slice(cut, d)) for p in range(2)]
    return jnp.concatenate([chain(slice(None), slice(0, cut)), jnp.concatenate(last, axis=0)], axis=1)


def attention(refs, out_ref, valid, heads, width):
    q_s, k_s, v_s, g_s = refs
    count = len(valid)
    seq = q_s.shape[0] // count
    lane_head = lax.broadcasted_iota(jnp.int32, (1, heads * width), 1) // width
    masks = [(lane_head == h).astype(BF16) for h in range(heads)]
    rows = [slice(b * seq, (b + 1) * seq) for b in range(count)]

    def blocks(x):
        return jnp.concatenate([x * m for m in masks], axis=0)

    def diagonal(full):
        out = full[:seq]
        for h in range(1, heads):
            out = jnp.where(lane_head == h, full[h * seq : (h + 1) * seq], out)
        return out

    scores = [dot_nt(k_s[r], blocks(q_s[r])) for r in rows]
    grad_prob = [dot_nt(v_s[r], blocks(g_s[r])) for r in rows]
    probs, grad_scores = [], []
    for score, grad, length in zip(scores, grad_prob, valid):
        row = lax.broadcasted_iota(jnp.int32, score.shape, 0)
        score = jnp.where(row < length, score, -1e30)
        exp_score = jnp.exp(score - jnp.max(score, axis=0, keepdims=True))
        prob = exp_score * (1.0 / jnp.sum(exp_score, axis=0, keepdims=True))
        probs.append(prob.astype(BF16))
        delta = jnp.sum(prob * grad, axis=0, keepdims=True)
        grad_scores.append((prob * (grad - delta)).astype(BF16))
    for r, prob, grad_score in zip(rows, probs, grad_scores):
        out_ref[2, r] = dot_nn(prob, blocks(g_s[r])).astype(BF16)
        out_ref[1, r] = dot_nn(grad_score, blocks(q_s[r])).astype(BF16)
        out_ref[3, r] = diagonal(dot_tn(prob, v_s[r])).astype(BF16)
        out_ref[0, r] = diagonal(dot_tn(grad_score, k_s[r])).astype(BF16)


def keep_rows(len_ref, first, count, seq):
    rows = [lax.broadcasted_iota(jnp.int32, (seq, 1), 0) < LEVELS * len_ref[first + b] for b in range(count)]
    return jnp.concatenate([r.astype(F32) for r in rows], axis=0)


def shard_body(len_ref, normed, mcot, w_q, w_k, w_v, w_o, out_ref, scratch, seq, heads, width):
    q_s, k_s, v_s, g_s = scratch
    chunk = pl.program_id(0)
    count = normed.shape[0] // seq
    q_s[...] = dot_nt(normed, w_q).astype(BF16)
    k_s[...] = dot_nt(normed, w_k).astype(BF16)
    v_s[...] = dot_nt(normed, w_v).astype(BF16)
    g_s[...] = dot_nt(mcot, w_o).astype(BF16)
    attention(scratch, out_ref, [LEVELS * len_ref[chunk * count + b] for b in range(count)], heads, width)


def own_kernel(seq, heads, width, len_ref, states_ref, cot_ref, gain_ref, qkv_ref, wo_ref,
               normed_ref, mcot_ref, out_ref, gain_out_ref, *scratch):
    wide = states_ref[...].astype(F32)
    inv = lax.rsqrt(jnp.mean(wide * wide, axis=-1, keepdims=True) + EPS)
    normed = (wide * inv * gain_ref[...]).astype(BF16)
    normed_ref[...] = normed
    count = normed.shape[0] // seq
    keep = keep_rows(len_ref, pl.program_id(0) * count, count, seq)
    mcot = (cot_ref[...].astype(F32) * keep).astype(BF16)
    mcot_ref[...] = mcot
    n = heads * width
    shard_body(len_ref, normed, mcot, qkv_ref[:n], qkv_ref[n : 2 * n], qkv_ref[2 * n : 3 * n], wo_ref[...],
               out_ref.at[:], scratch, seq, heads, width)

    @pl.when(pl.program_id(0) == 0)
    def _():
        gain_out_ref[...] = jnp.zeros_like(gain_out_ref)

    grad = project([(out_ref.at[i], qkv_ref.at[i * n : (i + 1) * n]) for i in range(3)])
    gain_out_ref[...] += jnp.sum(grad * (states_ref[...].astype(F32) * inv), axis=0, keepdims=True)


def far_kernel(seq, heads, width, len_ref, meta_ref, normed_ref, mcot_ref, *refs):
    blocks = refs[:2]
    out_ref, wt_ref, q_s, k_s, v_s, g_s, sems = refs[2:]
    n = heads * width

    @pl.when(pl.program_id(0) == 0)
    def _():
        copies = []
        for r in range(2):
            place = pl.multiple_of(((meta_ref[1] % 2) ^ r) * 2 * n, 8)
            copies.append(pltpu.make_async_copy(blocks[r], wt_ref.at[pl.ds(place, 2 * n)], sems.at[r]))
        for copy in copies:
            copy.start()
        for copy in copies:
            copy.wait()

    w = [wt_ref[i * n : (i + 1) * n] for i in range(4)]
    shard_body(len_ref, normed_ref[...], mcot_ref[...], w[0], w[1], w[2], w[3],
               out_ref.at[:], (q_s, k_s, v_s, g_s), seq, heads, width)


def weight_grad_kernel(parts, n, meta_ref, normed_ref, mcot_ref, all_ref, *refs):
    outs, acc = refs[:-1], refs[-1]
    step = pl.program_id(0)
    rows = normed_ref.shape[1]
    size = rows * pl.num_programs(0) // parts
    per = parts // 2
    for i in range(4):
        left = mcot_ref[...] if i == 3 else normed_ref[...]
        piece = dot_tn(left, all_ref[i])
        for c in range(per):
            acc[i, step * per + c] = piece[c * size : (c + 1) * size]

    @pl.when(step == pl.num_programs(0) - 1)
    def _():
        for r in range(parts):
            for i in range(4):
                value = acc[i, meta_ref[1] ^ r]
                if r % 2 == 0:
                    outs[r // 2][:, i * n : (i + 1) * n] = value
                else:
                    outs[per][r // 2, :, i * n : (i + 1) * n] = value.astype(BF16)


def final_kernel(seq, heads, width, parts, shards, len_ref, meta_ref, states_ref, normed_ref, mcot_ref, gain_ref,
                 all0_ref, all1_ref, qkv_ref, wo_ref, wt1_ref, *refs):
    blocks = refs[:parts]
    att_ref, grad_ref, wt_s, all_s = refs[parts : parts + 4]
    scratch, sems = refs[parts + 4 : -1], refs[-1]
    n = heads * width
    size = 4 * n // parts
    own = meta_ref[0]

    @pl.when(pl.program_id(0) == 0)
    def _():
        copies = [
            pltpu.make_async_copy(qkv_ref, wt_s.at[own, pl.ds(0, 3 * n)], sems.at[0]),
            pltpu.make_async_copy(wo_ref, wt_s.at[own, pl.ds(3 * n, n)], sems.at[1]),
            pltpu.make_async_copy(wt1_ref, wt_s.at[own ^ 1], sems.at[2]),
        ]
        for k in range(2, shards):
            for r in range(parts):
                place = pl.multiple_of((meta_ref[1] ^ r) * size, 8)
                copies.append(pltpu.make_async_copy(
                    blocks[r].at[k - 2], wt_s.at[own ^ k, pl.ds(place, size)], sems.at[3 + (k - 2) * parts + r]))
        for copy in copies:
            copy.start()
        for copy in copies:
            copy.wait()

    all_s[own] = all0_ref[...]
    all_s[own ^ 1] = all1_ref[...]
    normed, mcot = normed_ref[...], mcot_ref[...]
    count = normed.shape[0] // seq
    valid = [LEVELS * len_ref[pl.program_id(0) * count + b] for b in range(count)]
    for k in range(2, shards):
        for i in range(4):
            left = mcot if i == 3 else normed
            scratch[4 * (k % 2) + i][...] = dot_nt(left, wt_s[own ^ k, i * n : (i + 1) * n]).astype(BF16)
    for k in range(2, shards):
        attention(scratch[4 * (k % 2) : 4 * (k % 2) + 4], all_s.at[own ^ k], valid, heads, width)

    def piece(kind, shard):
        return all_s.at[shard, kind], wt_s.at[shard, kind * n : (kind + 1) * n]

    total = project([piece(3, s) for s in range(shards)])
    grad = project([piece(i, s) for s in range(shards) for i in range(3)])
    wide = states_ref[...].astype(F32)
    att_ref[...] = (wide + total).astype(BF16)
    inv = lax.rsqrt(jnp.mean(wide * wide, axis=-1, keepdims=True) + EPS)
    unit = wide * inv
    unit_grad = grad * gain_ref[...]
    corr = jnp.mean(unit_grad * unit, axis=-1, keepdims=True)
    grad_ref[...] = (mcot.astype(F32) + inv * (unit_grad - unit * corr)).astype(BF16)


def body(dp, mp, states, hist_len, norm_gain, qkv_weight, output_weight, cotangent):
    batch, seq, d = states.shape
    _, _, heads, width = qkv_weight.shape
    n = heads * width
    rows = batch * seq
    parts = 8
    low = dp // parts
    i_hi = lax.axis_index("dp") // low
    i_mp = lax.axis_index("mp")
    meta = jnp.stack([i_mp, i_hi]).astype(jnp.int32)

    def hop_dp(x, r):
        return lax.ppermute(x, "dp", [(i, i ^ (r * low)) for i in range(dp)])

    def hop_mp(x, k):
        return lax.ppermute(x, "mp", [(i, i ^ k) for i in range(mp)])

    qkv_rows = jnp.transpose(qkv_weight, (1, 2, 3, 0)).reshape(3 * n, d)
    wo_rows = output_weight.reshape(n, d)
    size = 4 * n // parts
    stacked = jnp.concatenate([qkv_rows, wo_rows], axis=0)
    mine = lax.dynamic_slice_in_dim(stacked, i_hi * size, size, 0)
    mine_near = lax.dynamic_slice_in_dim(stacked, (i_hi % 2) * 2 * n, 2 * n, 0)

    near = [hop_mp(mine_near, 1)]
    first = [hop_mp(mine, k) for k in range(2, mp)]
    near.append(hop_dp(near[0], 1))
    even = {0: jnp.stack(first)}
    for r in range(2, parts, 2):
        even[r] = hop_dp(even[0], r)
    blocks = dict(even)
    blocks[1] = hop_dp(even[0], 1)
    for r in range(2, parts, 2):
        blocks[r ^ 1] = hop_dp(even[r], 1)
    rest = [blocks[r] for r in range(parts)]

    flat_states = states.reshape(rows, d)
    flat_cot = cotangent.reshape(rows, d)
    gain = norm_gain.reshape(1, d)
    chunk = rows // 4
    grid = rows // chunk
    scratch = [pltpu.VMEM((chunk, n), BF16) for _ in range(8)]
    big_scratch = [pltpu.VMEM((rows // 2, n), BF16) for _ in range(4)]
    flops_in = 2 * rows * d * 4 * n
    big = rows // 2

    def row_of(size):
        return pl.BlockSpec((size, d), lambda c, *_: (c, 0))

    def all_of(size):
        return pl.BlockSpec((4, size, n), lambda c, *_: (0, c, 0))

    any_spec = pl.BlockSpec(memory_space=pl.ANY)
    all_shape = jax.ShapeDtypeStruct((4, rows, n), BF16)
    row_shape = jax.ShapeDtypeStruct((rows, d), BF16)

    def in_hbm(x):
        return pltpu.with_memory_space_constraint(x, pltpu.HBM)

    def whole(shape):
        return pl.BlockSpec(shape, lambda c, *_: tuple(0 for _ in shape))

    def call(kernel, flops, vmem, scalars, steps, in_specs, out_specs, out_shape, scratch_shapes):
        return pl.pallas_call(
            kernel, out_shape=out_shape,
            grid_spec=pltpu.PrefetchScalarGridSpec(
                num_scalar_prefetch=scalars, grid=(steps,), in_specs=in_specs, out_specs=out_specs,
                scratch_shapes=scratch_shapes),
            compiler_params=pltpu.CompilerParams(
                dimension_semantics=("arbitrary",), vmem_limit_bytes=vmem * 1024 * 1024),
            cost_estimate=pl.CostEstimate(flops=flops, bytes_accessed=rows * d * 8, transcendentals=0))

    normed, mcot, all0, gain_part = call(
        functools.partial(own_kernel, seq, heads, width), 3 * flops_in, 28, 1, 2,
        [row_of(big)] * 2 + [whole((1, d)), whole((3 * n, d)), whole((n, d))],
        [row_of(big)] * 2 + [all_of(big), whole((1, d))],
        [row_shape, row_shape, all_shape, jax.ShapeDtypeStruct((1, d), F32)], big_scratch,
    )(hist_len, in_hbm(flat_states), in_hbm(flat_cot), gain, qkv_rows, wo_rows)

    piece = (d // parts, 4 * n)
    half = parts // 2
    *kept, sent = call(
        functools.partial(weight_grad_kernel, parts, n), flops_in, 32, 1, 2,
        [pl.BlockSpec((rows, d // 2), lambda c, *_: (0, c))] * 2 + [whole((4, rows, n))],
        [whole(piece)] * half + [whole((half,) + piece)],
        [jax.ShapeDtypeStruct(piece, F32)] * half + [jax.ShapeDtypeStruct((half,) + piece, BF16)],
        [pltpu.VMEM((4, parts, d // parts, n), F32)],
    )(meta, normed, mcot, all0)
    others = []
    for k in range(1, mp):
        others.append(hop_mp(gain_part, k))
    all1, wt1 = call(
        functools.partial(far_kernel, seq, heads, width), 3 * flops_in, 28, 2, 2,
        [row_of(big)] * 2 + [any_spec] * 2,
        [all_of(big), whole((4 * n, d))], [all_shape, jax.ShapeDtypeStruct((4 * n, d), BF16)],
        big_scratch + [pltpu.SemaphoreType.DMA((2,))],
    )(hist_len, meta, normed, mcot, *near)

    all1, others = lax.optimization_barrier((all1, others))
    level = [gain_part] + others
    while len(level) > 1:
        level = [level[i] + level[i + 1] for i in range(0, len(level), 2)]
    gain_part = level[0]
    pair = hop_dp(sent, 1)
    gain_part = gain_part + hop_dp(gain_part, 1)
    kept = [kept[r] + pair[r].astype(F32) for r in range(half)]
    rounded = lax.reduce_precision(gain_part, 8, 7)
    tail = jnp.concatenate([rounded, gain_part - rounded, jnp.zeros((14, d), F32)], axis=0).astype(BF16)
    arrived = [
        hop_dp(jnp.concatenate([kept[r].astype(BF16), tail], axis=0), 2 * r) for r in range(1, half)
    ]

    attended, grad_states = call(
        functools.partial(final_kernel, seq, heads, width, parts, mp), 10 * flops_in, 30, 2, grid,
        [row_of(chunk)] * 3 + [whole((1, d)), all_of(chunk), all_of(chunk)] + [any_spec] * (3 + parts),
        [row_of(chunk)] * 2, [row_shape, row_shape],
        [pltpu.VMEM((mp, 4 * n, d), BF16), pltpu.VMEM((mp, 4, chunk, n), BF16)] + scratch
        + [pltpu.SemaphoreType.DMA((3 + (mp - 2) * parts,))],
    )(hist_len, meta, flat_states, normed, mcot, gain, all0, all1, qkv_rows, wo_rows, wt1, *rest)

    attended, arrived = lax.optimization_barrier((attended, arrived))
    summed, gain_sum = kept[0], gain_part
    for part in arrived:
        summed = summed + part[: d // parts].astype(F32)
        gain_sum = gain_sum + (part[d // parts].astype(F32) + part[d // parts + 1].astype(F32))
    gain_piece = lax.dynamic_slice_in_dim(gain_sum.reshape(d), i_hi * (d // parts), d // parts, 0)
    if low > 1:
        groups = [[hi * low + lo for lo in range(low)] for hi in range(parts)]
        summed = lax.psum_scatter(summed, "dp", scatter_dimension=0, axis_index_groups=groups, tiled=True)
        gain_piece = lax.psum_scatter(gain_piece, "dp", scatter_dimension=0, axis_index_groups=groups, tiled=True)
    across = summed.T
    grad_qkv = jnp.transpose(across[: 3 * n].reshape(3, heads, width, -1), (3, 0, 1, 2))
    grad_output = across[3 * n :].reshape(heads, width, -1)
    return (attended.reshape(batch, seq, d), grad_states.reshape(batch, seq, d), grad_qkv, grad_output, gain_piece)


def solution(mesh):
    placed = (
        P("dp", None, None),
        P("dp"),
        P(),
        P(None, None, "mp", None),
        P("mp", None, None),
        P("dp", None, None),
    )
    return jax.shard_map(
        functools.partial(body, mesh.shape["dp"], mesh.shape["mp"]),
        mesh=mesh,
        in_specs=placed,
        out_specs=(
            P("dp", None, None),
            P("dp", None, None),
            P("dp", None, "mp", None),
            P("mp", None, "dp"),
            P("dp"),
        ),
        check_vma=False,
    )
```
